32 devices in a mesh: gx: 4 (over z), gy: 8 (over y, x, core).
Axes of the slice: x: 2, y: 2, z: 4, core: 2. Of those that a mesh axis runs over, the one named last changes fastest.
Arguments:
- probes: float32 [8, 64, 128, 512], P(None, 'gx', 'gy'), may hold values from -12.5 to 12.5, as said below
- disorder: float32 [64, 128, 512], P('gx', 'gy'), may hold values from -2 to 2
- spectrum_center: float32 [1], replicated, may hold values from -0.5 to 0.5
- half_width: float32 [1], replicated, may hold values from 9 to 11
Outputs:
- last_vector: float32 [8, 64, 128, 512], P(None, 'gx', 'gy')
- moments: float32 [8, 8], replicated
The draws below stay inside these ranges and needn't reach their ends.
Inputs may be any that keep to these rules, and one draw needn't show every extreme that they name: `probes`: real-valued probe entries.
All inputs are finite; a program needn't handle non-finite values.
Results may differ from the reference program's by a relative error of at most 0.0001.
Values sent between devices are 32-bit elements; how exact they have to be, the bound alone decides.
A program may use at most 128 MiB of HBM per device.

```python
import jax
import jax.numpy as jnp

PROBES = 8
NZ = 512
STEPS = 4
NX = 64
NY = 128


def draw_probes(key, part):
    first, second = jax.random.split(key, 2)
    shape = (PROBES, NX, NY, NZ)
    rough = jnp.exp(jax.random.uniform(second, shape, jnp.float32, -0.7, 0.7))
    rows_x = jnp.arange(NX, dtype=jnp.float32)[:, None]
    rows_y = jnp.arange(NY, dtype=jnp.float32)[None, :]
    frac = (rows_x * NY + rows_y) / (NX * NY - 1.0)
    base = jnp.clip(jax.random.normal(first, shape, jnp.float32), -4.0, 4.0)
    ramp = 0.5 + frac
    return (base * rough * ramp[None, :, :, None]).astype(jnp.float32)


def block_scale(rng, dims, shards, smallest, high):
    loudness, own = 1.0, jax.random.fold_in(rng, 6)
    for dim, parts in shards:
        heights = jnp.exp(jax.random.uniform(jax.random.fold_in(own, dim), (parts,), jnp.float32, smallest / len(shards), high / len(shards)))
        loudness = loudness * jnp.repeat(heights, dims[dim] // parts).reshape([-1 if axis == dim else 1 for axis in range(len(dims))])
    return loudness


def setup_inputs(seed: int = 0) -> dict:
    key_of = jax.random.split(jax.random.key(seed), 5)
    return {
        "probes": draw_probes(jax.random.fold_in(key_of[4], 71), 0),
        "disorder": jnp.clip(jax.random.uniform(key_of[1], (NX, NY, NZ), jnp.float32, -2.0, 2.0) * block_scale(key_of[1], (NX, NY, NZ), ((0, 4), (1, 8)), -0.4, 0.0), -2.0, 2.0),
        "spectrum_center": jnp.clip(jax.random.uniform(key_of[2], (1,), jnp.float32, -0.5, 0.5), -0.5, 0.5),
        "half_width": jnp.clip(jax.random.uniform(key_of[3], (1,), jnp.float32, 9.0, 11.0), 9.0, 11.0),
    }


def scaled_apply(ext, eps_part, center, width):
    core = ext[:, 1:-1, 1:-1]
    beside = ext[:, 2:, 1:-1] + ext[:, :-2, 1:-1] + ext[:, 1:-1, 2:] + ext[:, 1:-1, :-2]
    beside = beside + jnp.roll(core, 1, 3) + jnp.roll(core, -1, 3)
    return ((eps_part - center) * core - beside) / width


def padded(field):
    return jnp.pad(field, ((0, 0), (1, 1), (1, 1), (0, 0)), mode="wrap")


def inner_pair(t_low, t_high):
    square = jnp.sum(t_low * t_low, axis=(1, 2, 3))
    cross = jnp.sum(t_high * t_low, axis=(1, 2, 3))
    return jnp.stack([square, cross])


def reference(probes, disorder, spectrum_center, half_width):
    center = spectrum_center[0]
    width = half_width[0]
    energy = disorder[None]
    t_low = probes
    t_high = scaled_apply(padded(t_low), energy, center, width)
    collected = []
    for step in range(STEPS):
        collected.append(inner_pair(t_low, t_high))
        if step + 1 < STEPS:
            t_next = 2.0 * scaled_apply(padded(t_high), energy, center, width) - t_low
            t_low, t_high = t_high, t_next
    stacked = jnp.stack(collected)
    sites = jnp.float32(NX * NY * NZ)
    square = stacked[:, 0, :] / sites
    cross = stacked[:, 1, :] / sites
    even = 2.0 * square - square[0]
    odd = 2.0 * cross - cross[0]
    moments = jnp.stack([even, odd], axis=1).reshape(2 * STEPS, -1).T
    return t_high, moments
```

```python
import functools

import jax
import jax.numpy as jnp
from jax import lax
from jax.experimental import pallas as pl
from jax.experimental.pallas import tpu as pltpu
from jax.sharding import PartitionSpec as P

STEPS = 4
MESH = pl.DeviceIdType.MESH
ROWS = 8


def kernel(counts, sites, probes_hbm, disorder, center, width, last, moments, *scratch):
    fields = scratch[:STEPS]
    (near, faces, coef, acc, gather_x, gather_y, load_sem, send_sem, recv_sem,
     xs_sem, xr_sem, ys_sem, yr_sem) = scratch[STEPS:]
    n_probes, nx, ny, nz = probes_hbm.shape
    tiles = ny // ROWS
    count_x, count_y = counts
    me_x = lax.axis_index("gx")
    me_y = lax.axis_index("gy")

    def at_x(offset):
        return (lax.rem(me_x + offset, count_x), me_y)

    def at_y(offset):
        return (me_x, lax.rem(me_y + offset, count_y))

    def load(p):
        return pltpu.make_async_copy(
            probes_hbm.at[p], fields[0].at[p, pl.ds(1, nx)], load_sem.at[p])

    def x_sends(s, p):
        if s == 0:
            low, high = probes_hbm.at[p, 0], probes_hbm.at[p, nx - 1]
        else:
            low, high = fields[s].at[p, 1], fields[s].at[p, nx]
        return (
            pltpu.make_async_remote_copy(
                low, fields[s].at[p, nx + 1], send_sem.at[s, p, 0], recv_sem.at[s, p, 0],
                device_id=at_x(count_x - 1), device_id_type=MESH),
            pltpu.make_async_remote_copy(
                high, fields[s].at[p, 0], send_sem.at[s, p, 1], recv_sem.at[s, p, 1],
                device_id=at_x(1), device_id_type=MESH),
        )

    def y_sends(s, p):
        return (
            pltpu.make_async_remote_copy(
                faces.at[s, 0, p], near.at[s, 1, p], send_sem.at[s, p, 2], recv_sem.at[s, p, 2],
                device_id=at_y(count_y - 1), device_id_type=MESH),
            pltpu.make_async_remote_copy(
                faces.at[s, 1, p], near.at[s, 0, p], send_sem.at[s, p, 3], recv_sem.at[s, p, 3],
                device_id=at_y(1), device_id_type=MESH),
        )

    @pl.loop(0, n_probes)
    def _(p):
        load(p).start()

    barrier = pltpu.get_barrier_semaphore()
    for offset in range(1, count_x):
        pl.semaphore_signal(barrier, inc=1, device_id=at_x(offset), device_id_type=MESH)
    for offset in range(1, count_y):
        pl.semaphore_signal(barrier, inc=1, device_id=at_y(offset), device_id_type=MESH)

    scale = 2.0 / jnp.full((ROWS, nz), width[0], jnp.float32)
    middle = center[0]

    @pl.loop(0, nx)
    def _(x):
        for i in range(tiles):
            part = pl.ds(ROWS * i, ROWS)
            coef[x, part] = (disorder[x, part] - middle) * scale

    pl.semaphore_wait(barrier, count_x + count_y - 2)

    @pl.loop(0, n_probes)
    def _(p):
        for copy in x_sends(0, p):
            copy.start()

    @pl.loop(0, n_probes)
    def _(p):
        load(p).wait()

        @pl.loop(0, nx)
        def _(x):
            faces[0, 0, p, x] = fields[0][p, x + 1, pl.ds(0, 1)]
            faces[0, 1, p, x] = fields[0][p, x + 1, pl.ds(ny - 1, 1)]

        for copy in y_sends(0, p):
            copy.start()

    sub = lax.broadcasted_iota(jnp.int32, (ROWS, nz), 0)
    first = sub == 0
    final = sub == ROWS - 1
    lanes = lax.broadcasted_iota(jnp.int32, (n_probes, 128), 1)
    sums = jnp.zeros((n_probes, 128), jnp.float32)

    def fold(v):
        parts = [v[:, 128 * j:128 * (j + 1)] for j in range(nz // 128)]
        while len(parts) > 1:
            parts = [a + b for a, b in zip(parts[::2], parts[1::2])] + (
                [parts[-1]] if len(parts) % 2 else [])
        return parts[0]

    for s in range(STEPS):
        cur = fields[s]

        @pl.loop(0, n_probes)
        def _(p):
            for copy in x_sends(s, p) + y_sends(s, p):
                copy.wait_recv()

            def row(x, carry):
                square, cross = carry
                low = jnp.broadcast_to(near[s, 0, p, x], (ROWS, nz))
                high = jnp.broadcast_to(near[s, 1, p, x], (ROWS, nz))
                here = [cur[p, x + 1, pl.ds(ROWS * i, ROWS)] for i in range(tiles)]
                down = [pltpu.roll(v, 1, 0) for v in here]
                up = [pltpu.roll(v, ROWS - 1, 0) for v in here]
                for i in range(tiles):
                    part = pl.ds(ROWS * i, ROWS)
                    v = here[i]
                    below = jnp.where(first, low if i == 0 else down[i - 1], down[i])
                    above = jnp.where(final, high if i == tiles - 1 else up[i + 1], up[i])
                    beside = cur[p, x, part] + cur[p, x + 2, part]
                    beside = beside + (below + above)
                    beside = beside + (pltpu.roll(v, 1, 1) + pltpu.roll(v, nz - 1, 1))
                    new = coef[x, part] * v - scale * beside
                    if s == 0:
                        new = 0.5 * new
                    else:
                        new = new - fields[s - 1][p, x + 1, part]
                    if s + 1 < STEPS:
                        fields[s + 1][p, x + 1, part] = new
                        if i == 0:
                            faces[s + 1, 0, p, x] = new[0:1]
                        if i == tiles - 1:
                            faces[s + 1, 1, p, x] = new[ROWS - 1:ROWS]
                    else:
                        last[p, x, part] = new
                    square = square + fold(v * v)
                    cross = cross + fold(new * v)
                return square, cross

            zero = jnp.zeros((ROWS, 128), jnp.float32)
            square, cross = lax.fori_loop(0, nx, row, (zero, zero))
            acc[0, p] = square
            acc[1, p] = cross
            if s + 1 < STEPS:
                for copy in x_sends(s + 1, p) + y_sends(s + 1, p):
                    copy.start()

        for k in range(2):
            total = jnp.sum(jnp.sum(acc[k], axis=1), axis=1, keepdims=True)
            sums = sums + jnp.where(lanes == 2 * s + k, total, 0.0)

    def reduce_over(value, gather, sends, recvs, me, count, where):
        gather[me] = value

        def send(offset):
            return pltpu.make_async_remote_copy(
                gather.at[me], gather.at[me], sends.at[offset], recvs.at[me],
                device_id=where(offset), device_id_type=MESH)

        for offset in range(1, count):
            send(offset).start()
        for offset in range(1, count):
            source = lax.rem(me + offset, count)
            pltpu.make_async_remote_copy(
                gather.at[source], gather.at[source], sends.at[offset], recvs.at[source],
                device_id=where(offset), device_id_type=MESH).wait_recv()
        total = gather[0]
        for k in range(1, count):
            total = total + gather[k]
        return total, send

    sums, send_x = reduce_over(sums, gather_x, xs_sem, xr_sem, me_x, count_x, at_x)
    sums, send_y = reduce_over(sums, gather_y, ys_sem, yr_sem, me_y, count_y, at_y)
    mean = sums / jnp.float32(sites)
    start = jnp.where(lax.rem(lanes, 2) == 0, mean[:, 0:1], mean[:, 1:2])
    moments[...] = (2.0 * mean - start)[:, :2 * STEPS]

    for offset in range(1, count_x):
        send_x(offset).wait_send()
    for offset in range(1, count_y):
        send_y(offset).wait_send()
    for s in range(STEPS):
        @pl.loop(0, n_probes)
        def _(p):
            for copy in x_sends(s, p) + y_sends(s, p):
                copy.wait_send()


def local(counts, probes, disorder, spectrum_center, half_width):
    n_probes, nx, ny, nz = probes.shape
    sites = nx * counts[0] * ny * counts[1] * nz
    f32 = jnp.float32
    dma = pltpu.SemaphoreType.DMA
    vmem = pl.BlockSpec(memory_space=pltpu.VMEM)
    smem = pl.BlockSpec(memory_space=pltpu.SMEM)
    return pl.pallas_call(
        functools.partial(kernel, counts, sites),
        out_shape=(
            jax.ShapeDtypeStruct(probes.shape, f32),
            jax.ShapeDtypeStruct((n_probes, 2 * STEPS), f32),
        ),
        in_specs=[pl.BlockSpec(memory_space=pl.ANY), vmem, smem, smem],
        out_specs=(vmem, vmem),
        scratch_shapes=[pltpu.VMEM((n_probes, nx + 2, ny, nz), f32)] * STEPS + [
            pltpu.VMEM((STEPS, 2, n_probes, nx, 1, nz), f32),
            pltpu.VMEM((STEPS, 2, n_probes, nx, 1, nz), f32),
            pltpu.VMEM((nx, ny, nz), f32),
            pltpu.VMEM((2, n_probes, ROWS, 128), f32),
            pltpu.VMEM((counts[0], n_probes, 128), f32),
            pltpu.VMEM((counts[1], n_probes, 128), f32),
            dma((n_probes,)),
            dma((STEPS, n_probes, 4)),
            dma((STEPS, n_probes, 4)),
            dma((counts[0],)),
            dma((counts[0],)),
            dma((counts[1],)),
            dma((counts[1],)),
        ],
        compiler_params=pltpu.CompilerParams(
            collective_id=0, has_side_effects=True, vmem_limit_bytes=58 * 1024 * 1024),
        name="moments",
    )(probes, disorder, spectrum_center, half_width)


def solution(mesh):
    counts = (mesh.shape["gx"], mesh.shape["gy"])
    in_specs = (P(None, "gx", "gy", None), P("gx", "gy", None), P(), P())
    out_specs = (P(None, "gx", "gy", None), P())
    return jax.shard_map(functools.partial(local, counts), mesh=mesh, in_specs=in_specs,
                         out_specs=out_specs, check_vma=False)
```

```python
import functools

import jax
import jax.numpy as jnp
from jax import lax
from jax.experimental import pallas as pl
from jax.experimental.pallas import tpu as pltpu
from jax.sharding import PartitionSpec as P

STEPS = 4
MESH = pl.DeviceIdType.MESH
ROWS = 8


def kernel(counts, sites, probes_hbm, disorder_hbm, center, width, last_hbm, moments, *scratch):
    fields = scratch[:STEPS]
    (last, disorder, near, faces, coef, acc, gather_x, gather_y, load_sem, out_sem, energy_sem, send_sem, recv_sem,
     xs_sem, xr_sem, ys_sem, yr_sem) = scratch[STEPS:]
    n_probes, nx, ny, nz = probes_hbm.shape
    tiles = ny // ROWS
    count_x, count_y = counts
    me_x = lax.axis_index("gx")
    me_y = lax.axis_index("gy")

    def at_x(offset):
        return (lax.rem(me_x + offset, count_x), me_y)

    def at_y(offset):
        return (me_x, lax.rem(me_y + offset, count_y))

    def load(p):
        return pltpu.make_async_copy(
            probes_hbm.at[p], fields[0].at[p, pl.ds(1, nx)], load_sem.at[p])

    def store(p):
        return pltpu.make_async_copy(last.at[p], last_hbm.at[p], out_sem.at[p])

    def x_sends(s, p):
        if s == 0:
            low, high = probes_hbm.at[p, 0], probes_hbm.at[p, nx - 1]
        else:
            low, high = fields[s].at[p, 1], fields[s].at[p, nx]
        return (
            pltpu.make_async_remote_copy(
                low, fields[s].at[p, nx + 1], send_sem.at[s, p, 0], recv_sem.at[s, p, 0],
                device_id=at_x(count_x - 1), device_id_type=MESH),
            pltpu.make_async_remote_copy(
                high, fields[s].at[p, 0], send_sem.at[s, p, 1], recv_sem.at[s, p, 1],
                device_id=at_x(1), device_id_type=MESH),
        )

    def y_sends(s, p):
        return (
            pltpu.make_async_remote_copy(
                faces.at[s, 0, p], near.at[s, 1, p], send_sem.at[s, p, 2], recv_sem.at[s, p, 2],
                device_id=at_y(count_y - 1), device_id_type=MESH),
            pltpu.make_async_remote_copy(
                faces.at[s, 1, p], near.at[s, 0, p], send_sem.at[s, p, 3], recv_sem.at[s, p, 3],
                device_id=at_y(1), device_id_type=MESH),
        )

    barrier = pltpu.get_barrier_semaphore()
    for offset in range(1, count_x):
        pl.semaphore_signal(barrier, inc=1, device_id=at_x(offset), device_id_type=MESH)
    for offset in range(1, count_y):
        pl.semaphore_signal(barrier, inc=1, device_id=at_y(offset), device_id_type=MESH)

    @pl.loop(0, n_probes)
    def _(p):
        load(p).start()

    energy = pltpu.make_async_copy(disorder_hbm, disorder, energy_sem)
    energy.start()
    scale = 2.0 / jnp.full((ROWS, nz), width[0], jnp.float32)
    middle = center[0]

    pl.semaphore_wait(barrier, count_x + count_y - 2)

    @pl.loop(0, n_probes)
    def _(p):
        for copy in x_sends(0, p):
            copy.start()

    @pl.loop(0, n_probes)
    def _(p):
        load(p).wait()

        @pl.loop(0, nx)
        def _(x):
            faces[0, 0, p, x] = fields[0][p, x + 1, pl.ds(0, 1)]
            faces[0, 1, p, x] = fields[0][p, x + 1, pl.ds(ny - 1, 1)]

        for copy in y_sends(0, p):
            copy.start()

    energy.wait()

    @pl.loop(0, nx)
    def _(x):
        for i in range(tiles):
            part = pl.ds(ROWS * i, ROWS)
            coef[x, part] = (disorder[x, part] - middle) * scale

    sub = lax.broadcasted_iota(jnp.int32, (ROWS, nz), 0)
    first = sub == 0
    final = sub == ROWS - 1
    lanes = lax.broadcasted_iota(jnp.int32, (n_probes, 128), 1)
    sums = jnp.zeros((n_probes, 128), jnp.float32)

    def fold(v):
        parts = [v[:, 128 * j:128 * (j + 1)] for j in range(nz // 128)]
        while len(parts) > 1:
            parts = [a + b for a, b in zip(parts[::2], parts[1::2])] + (
                [parts[-1]] if len(parts) % 2 else [])
        return parts[0]

    for s in range(STEPS):
        cur = fields[s]

        @pl.loop(0, n_probes)
        def _(p):
            for copy in x_sends(s, p) + y_sends(s, p):
                copy.wait_recv()

            def row(x, carry):
                square, cross = carry
                low = jnp.broadcast_to(near[s, 0, p, x], (ROWS, nz))
                high = jnp.broadcast_to(near[s, 1, p, x], (ROWS, nz))
                here = [cur[p, x + 1, pl.ds(ROWS * i, ROWS)] for i in range(tiles)]
                down = [pltpu.roll(v, 1, 0) for v in here]
                up = [pltpu.roll(v, ROWS - 1, 0) for v in here]
                for i in range(tiles):
                    part = pl.ds(ROWS * i, ROWS)
                    v = here[i]
                    below = jnp.where(first, low if i == 0 else down[i - 1], down[i])
                    above = jnp.where(final, high if i == tiles - 1 else up[i + 1], up[i])
                    beside = cur[p, x, part] + cur[p, x + 2, part]
                    beside = beside + (below + above)
                    beside = beside + (pltpu.roll(v, 1, 1) + pltpu.roll(v, nz - 1, 1))
                    new = coef[x, part] * v - scale * beside
                    if s == 0:
                        new = 0.5 * new
                    else:
                        new = new - fields[s - 1][p, x + 1, part]
                    if s + 1 < STEPS:
                        fields[s + 1][p, x + 1, part] = new
                        if i == 0:
                            faces[s + 1, 0, p, x] = new[0:1]
                        if i == tiles - 1:
                            faces[s + 1, 1, p, x] = new[ROWS - 1:ROWS]
                    else:
                        last[p, x, part] = new
                    square = square + fold(v * v)
                    cross = cross + fold(new * v)
                return square, cross

            zero = jnp.zeros((ROWS, 128), jnp.float32)
            square, cross = lax.fori_loop(0, nx, row, (zero, zero), unroll=16)
            acc[0, p] = square
            acc[1, p] = cross
            if s + 1 < STEPS:
                for copy in x_sends(s + 1, p) + y_sends(s + 1, p):
                    copy.start()
            else:
                store(p).start()
            for copy in x_sends(s, p) + y_sends(s, p):
                copy.wait_send()

        for k in range(2):
            total = jnp.sum(jnp.sum(acc[k], axis=1), axis=1, keepdims=True)
            sums = sums + jnp.where(lanes == 2 * s + k, total, 0.0)

    def reduce_over(value, gather, sends, recvs, me, count, where):
        gather[me] = value

        def send(offset):
            return pltpu.make_async_remote_copy(
                gather.at[me], gather.at[me], sends.at[offset], recvs.at[me],
                device_id=where(offset), device_id_type=MESH)

        for offset in range(1, count):
            send(offset).start()
        for offset in range(1, count):
            source = lax.rem(me + offset, count)
            pltpu.make_async_remote_copy(
                gather.at[source], gather.at[source], sends.at[offset], recvs.at[source],
                device_id=where(offset), device_id_type=MESH).wait_recv()
        total = gather[0]
        for k in range(1, count):
            total = total + gather[k]
        return total, send

    sums, send_x = reduce_over(sums, gather_x, xs_sem, xr_sem, me_x, count_x, at_x)
    sums, send_y = reduce_over(sums, gather_y, ys_sem, yr_sem, me_y, count_y, at_y)
    mean = sums / jnp.float32(sites)
    start = jnp.where(lax.rem(lanes, 2) == 0, mean[:, 0:1], mean[:, 1:2])
    moments[...] = (2.0 * mean - start)[:, :2 * STEPS]

    for offset in range(1, count_x):
        send_x(offset).wait_send()
    for offset in range(1, count_y):
        send_y(offset).wait_send()

    @pl.loop(0, n_probes)
    def _(p):
        store(p).wait()


def local(counts, probes, disorder, spectrum_center, half_width):
    n_probes, nx, ny, nz = probes.shape
    sites = nx * counts[0] * ny * counts[1] * nz
    f32 = jnp.float32
    dma = pltpu.SemaphoreType.DMA
    vmem = pl.BlockSpec(memory_space=pltpu.VMEM)
    hbm = pl.BlockSpec(memory_space=pl.ANY)
    smem = pl.BlockSpec(memory_space=pltpu.SMEM)
    return pl.pallas_call(
        functools.partial(kernel, counts, sites),
        out_shape=(
            jax.ShapeDtypeStruct(probes.shape, f32),
            jax.ShapeDtypeStruct((n_probes, 2 * STEPS), f32),
        ),
        in_specs=[hbm, hbm, smem, smem],
        out_specs=(hbm, vmem),
        scratch_shapes=[pltpu.VMEM((n_probes, nx + 2, ny, nz), f32)] * STEPS + [
            pltpu.VMEM(probes.shape, f32),
            pltpu.VMEM((nx, ny, nz), f32),
            pltpu.VMEM((STEPS, 2, n_probes, nx, 1, nz), f32),
            pltpu.VMEM((STEPS, 2, n_probes, nx, 1, nz), f32),
            pltpu.VMEM((nx, ny, nz), f32),
            pltpu.VMEM((2, n_probes, ROWS, 128), f32),
            pltpu.VMEM((counts[0], n_probes, 128), f32),
            pltpu.VMEM((counts[1], n_probes, 128), f32),
            dma((n_probes,)),
            dma((n_probes,)),
            dma,
            dma((STEPS, n_probes, 4)),
            dma((STEPS, n_probes, 4)),
            dma((counts[0],)),
            dma((counts[0],)),
            dma((counts[1],)),
            dma((counts[1],)),
        ],
        compiler_params=pltpu.CompilerParams(
            collective_id=0, has_side_effects=True, vmem_limit_bytes=58 * 1024 * 1024),
        name="moments",
    )(probes, disorder, spectrum_center, half_width)


def solution(mesh):
    counts = (mesh.shape["gx"], mesh.shape["gy"])
    in_specs = (P(None, "gx", "gy", None), P("gx", "gy", None), P(), P())
    out_specs = (P(None, "gx", "gy", None), P())
    return jax.shard_map(functools.partial(local, counts), mesh=mesh, in_specs=in_specs,
                         out_specs=out_specs, check_vma=False)
```
